32 devices in a mesh: groups: 2 (over x), seq: 16 (over z, y, core).
Axes of the slice: x: 2, y: 2, z: 4, core: 2. Of those that a mesh axis runs over, the one named last changes fastest.
Arguments:
- queries: bfloat16 [8192, 4096], P(('groups', 'seq')), parts along dimension 0, may hold values from -6 to 6
- keys: bfloat16 [8192, 2048], P(('groups', 'seq')), parts along dimension 0, may hold values from -6 to 6
- values: bfloat16 [8192, 2048], P(('groups', 'seq')), parts along dimension 0, may hold values from -6 to 6
- doc_blocks: int32 [16], P('groups'), parts along dimension 0, may hold values from 1 to 8, 32 in all
Outputs:
- attended: bfloat16 [8192, 4096], P(('groups', 'seq')), parts along dimension 0
The draws below stay inside these ranges and needn't reach their ends.
There are 2 independent parts, one for each index of `groups`. The reference program is written for one: setup_inputs(seed, part) draws one part's arguments, and reference() takes and returns one part's arrays. A program takes and returns all parts, laid end to end along the dimension named above; each array names one. Nothing has to cross between parts.
Inputs may be any that keep to these rules, and one draw needn't show every extreme that they name: `doc_blocks`: the lengths add up to 32; the longest document has exactly 8 units.
All inputs are finite; a program needn't handle non-finite values.
Results may differ from the reference program's by a relative error of at most 0.004.
Values may be sent and summed in bfloat16 or wider, within the bound.
A program may use at most 64 MiB of HBM per device.

```python
import math
import jax
import jax.numpy as jnp
import numpy as np
from jax import lax

HEADS = 32
KV_HEADS = 16
DH = 128
BLK = 128
DOCS = 8
TOKENS = 4096


def draw_keys(key, part):
    own_key = jax.random.fold_in(key, 11)
    background = jnp.clip(jax.random.normal(own_key, (TOKENS, KV_HEADS * DH), jnp.float32), -6.0, 6.0)
    return background.astype(jnp.bfloat16)


def draw_queries(key, part):
    own_key = jax.random.fold_in(key, 17)
    background = jnp.clip(jax.random.normal(own_key, (TOKENS, HEADS * DH), jnp.float32), -6.0, 6.0)
    return background.astype(jnp.bfloat16)


def levels(key, dims, pieces, low, high):
    def one(dim, shards_of):
        draws = jax.random.uniform(jax.random.fold_in(jax.random.fold_in(key, 6), dim), (shards_of,), jnp.float32, low / len(pieces), high / len(pieces))
        return jnp.repeat(jnp.exp(draws), dims[dim] // shards_of).reshape((-1,) + (1,) * (len(dims) - dim - 1))

    loudness = one(*pieces[0])
    for cut in pieces[1:]:
        loudness = loudness * one(*cut)
    return loudness


def length_profile(amount, total, most, slope):
    portions = [(1 << 20) // math.isqrt(rank ** slope) + 1 for rank in range(2, amount + 1)]
    spare, counts = total - most - (amount - 1), [1] * (amount - 1)
    while spare > 0:
        movable = [i for i in range(amount - 1) if counts[i] < most]
        mass, budget = sum([portions[i] for i in movable]), spare
        for i in movable:
            extra = min(most - counts[i], max(1, budget * portions[i] // mass), spare)
            counts[i] = counts[i] + extra
            spare = spare - extra
    return np.array([most] + counts)


def ragged_sizes(stream_key, number_of, total, limit, lean):
    if number_of == 2:
        one = jax.random.randint(stream_key, (), max(1, total - limit), min(limit, total - 1) + 1)
        return jnp.stack([one, total - one])
    tallies = jnp.asarray(length_profile(number_of, total, limit, lean), jnp.int32)
    twos = (number_of - 1) // 2
    source_of, sink = tallies[1:1 + 2 * twos:2], tallies[2:2 + 2 * twos:2]
    margin = jnp.minimum(source_of - 1, limit - sink)
    shifted = jax.random.randint(jax.random.fold_in(stream_key, 1), (twos,), 0, 1 << 20) % (margin + 1)
    tallies = tallies.at[1:1 + 2 * twos:2].set(source_of - shifted).at[2:2 + 2 * twos:2].set(sink + shifted)
    return tallies[jax.random.permutation(jax.random.fold_in(stream_key, 2), number_of)]


def bell_draw(key, dims, width, most, pieces=(), held_as=jnp.bfloat16):
    gain = levels(key, dims, pieces, -0.22, 0.18) if pieces else 1.0
    entries = jax.random.normal(key, dims, jnp.float32) * width * gain
    return jnp.minimum(jnp.maximum(entries, -most), most).astype(held_as)


def setup_inputs(seed: int = 0, part: int = 0) -> dict:
    key_list = jax.random.split(jax.random.key(seed), 5)
    own_keys = jax.random.split(jax.random.fold_in(key_list[4], part), 5)
    queries = draw_queries(jax.random.fold_in(jax.random.fold_in(key_list[4], part), 71), part)
    keys = draw_keys(jax.random.fold_in(jax.random.fold_in(key_list[4], part), 71), part)
    values = bell_draw(own_keys[2], (TOKENS, KV_HEADS * DH), 1.0, 6.0, ((0, 16),))
    doc_blocks = ragged_sizes(own_keys[3], DOCS, TOKENS // BLK, TOKENS // BLK // 4, 2).astype(jnp.int32)
    return dict(queries=queries, keys=keys, values=values, doc_blocks=doc_blocks)


score_scale = 144.0 ** -0.5


def reference(queries, keys, values, doc_blocks):
    lengths = doc_blocks.astype(jnp.int32) * BLK
    doc_ends = jnp.cumsum(lengths).astype(jnp.int32)
    doc_starts = (doc_ends - lengths).astype(jnp.int32)
    positions = jnp.arange(TOKENS, dtype=jnp.int32)
    doc_number = jnp.sum((positions[:, None] >= doc_ends[None, :]).astype(jnp.int32), axis=1).astype(jnp.int32)
    own_start = jnp.sum(jnp.where(doc_number[:, None] == jnp.arange(DOCS, dtype=jnp.int32)[None, :], doc_starts[None, :], 0), axis=1).astype(jnp.int32)
    query_heads = queries.reshape(TOKENS, KV_HEADS, HEADS // KV_HEADS, DH)
    key_heads = keys.reshape(TOKENS, KV_HEADS, DH)
    value_heads = values.reshape(TOKENS, KV_HEADS, DH)
    tile_rows = min(256, TOKENS)
    window_rows = min(TOKENS, TOKENS // 4 + tile_rows)

    def one_tile(block_index):
        first_row = (block_index * tile_rows).astype(jnp.int32)
        query_tile = lax.dynamic_slice_in_dim(query_heads, first_row, tile_rows, 0).astype(jnp.float32)
        key_first = jnp.clip(first_row + tile_rows - window_rows, 0, TOKENS - window_rows).astype(jnp.int32)
        key_tile = lax.dynamic_slice_in_dim(key_heads, key_first, window_rows, 0).astype(jnp.float32)
        value_tile = lax.dynamic_slice_in_dim(value_heads, key_first, window_rows, 0).astype(jnp.float32)
        scores = jnp.einsum("qgsd,kgd->gsqk", query_tile, key_tile) * score_scale
        tile_pos = first_row + jnp.arange(tile_rows, dtype=jnp.int32)
        tile_start = lax.dynamic_slice_in_dim(own_start, first_row, tile_rows, 0)
        key_pos = key_first + jnp.arange(window_rows, dtype=jnp.int32)
        visible = (key_pos[None, :] >= tile_start[:, None]) & (key_pos[None, :] <= tile_pos[:, None])
        row_max = jnp.max(jnp.where(visible, scores, -1e30), axis=-1)
        weights = jnp.where(visible, jnp.exp(scores - row_max[..., None]), 0.0)
        row_total = jnp.sum(weights, axis=-1)
        rounded = lax.optimization_barrier(weights.astype(jnp.bfloat16)).astype(jnp.float32)
        blended = jnp.einsum("gsqk,kgd->gsqd", rounded, value_tile) / row_total[..., None]
        return blended.transpose(2, 0, 1, 3).reshape(tile_rows, HEADS * DH).astype(jnp.bfloat16)

    blocks = lax.map(one_tile, jnp.arange(TOKENS // tile_rows, dtype=jnp.int32))
    return blocks.reshape(TOKENS, HEADS * DH)
```

```python
import functools

import jax
import jax.numpy as jnp
from jax import lax
from jax.experimental import pallas as pl
from jax.experimental.pallas import tpu as pltpu
from jax.sharding import PartitionSpec as P

DH = 128
BLK = 128
CHUNK_HEADS = 1
EXP2_SCALE = 144.0 ** (-0.5) * 1.4426950408889634
HIDDEN = -1e30


def kernel(
    n,
    window,
    docs_ref,
    q_hbm,
    k_hbm,
    v_hbm,
    o_hbm,
    q_own,
    k_own,
    v_own,
    k_halo,
    v_halo,
    o_own,
    local_sem,
    out_sem,
    send_sem,
    recv_sem,
):
    me = lax.axis_index("seq")
    pairs = window // 2
    place = lax.rem(me, window)
    base = me - place
    pair = place // 2
    core = lax.rem(me, 2)
    partner = me + 1 - 2 * core
    above = lax.rem(me + window, n)
    below = lax.rem(me + n - window, n)

    rows, kv_width = k_hbm.shape
    ratio = q_hbm.shape[1] // kv_width
    width = CHUNK_HEADS * DH
    chunks = kv_width // width
    blocks = rows // BLK
    own_hbm = (k_hbm, v_hbm)
    halo = (k_halo, v_halo)

    def pair_device(step):
        return base + 2 * lax.rem(pair + step, pairs) + core

    def kv_cols(c):
        return pl.ds(pl.multiple_of(c * width, width), width)

    def q_cols(c):
        return pl.ds(pl.multiple_of(c * width * ratio, width * ratio), width * ratio)

    def remote(c, src_slot, dst_slot, device):
        copies = []
        for kind in range(2):
            if src_slot is None:
                src = own_hbm[kind].at[:, kv_cols(c)]
            else:
                src = halo[kind].at[src_slot, :, kv_cols(c)]
            copies.append(
                pltpu.make_async_remote_copy(
                    src_ref=src,
                    dst_ref=halo[kind].at[dst_slot, :, kv_cols(c)],
                    send_sem=send_sem.at[kind, dst_slot, c],
                    recv_sem=recv_sem.at[kind, dst_slot, c],
                    device_id={"seq": device},
                    device_id_type=pl.DeviceIdType.MESH,
                )
            )
        return copies

    def start(copies):
        for copy in copies:
            copy.start()

    def partner_slot(step):
        return lax.rem(2 * step + 1 - 2 * core + window, window)

    barrier = pltpu.get_barrier_semaphore()
    greet = [above, below, partner] + [pair_device(step) for step in range(1, pairs)]
    for device in greet:
        pl.semaphore_signal(
            barrier, inc=1, device_id={"seq": device}, device_id_type=pl.DeviceIdType.MESH
        )
    local = [
        pltpu.make_async_copy(k_hbm, k_own, local_sem.at[0]),
        pltpu.make_async_copy(v_hbm, v_own, local_sem.at[1]),
        pltpu.make_async_copy(q_hbm, q_own, local_sem.at[2]),
    ]
    start(local)
    pl.semaphore_wait(barrier, len(greet))

    def first_sends(c, carry):
        start(remote(c, None, 0, above))
        for step in range(1, pairs):

            @pl.when(pair + step < pairs)
            def _():
                start(remote(c, None, 2 * step, pair_device(step)))

        @pl.when(core == 0)
        def _():
            start(remote(c, None, 1, partner))

        return carry

    lax.fori_loop(0, chunks, first_sends, 0)

    hide_rows = []
    for a in range(blocks):
        number = me * blocks + a
        end = jnp.int32(0)
        first = jnp.int32(0)
        for d in range(docs_ref.shape[0]):
            end = end + docs_ref[d]
            first = jnp.where(end <= number, end, first)
        held = [(me - window) * blocks + b for b in range(a + 1, blocks)]
        for r in range(1, window):
            held += [(me - r) * blocks + b for b in range(blocks)]
        held += [me * blocks + b for b in range(a + 1)]
        hide_rows.append(
            jnp.concatenate(
                [
                    jnp.full((1, BLK), jnp.where(b >= first, 0.0, HIDDEN), jnp.float32)
                    for b in held
                ],
                axis=1,
            )
        )

    for copy in local:
        copy.wait()

    def attend(c):
        q_index = lax.broadcasted_iota(jnp.int32, (BLK, BLK), 0)
        k_index = lax.broadcasted_iota(jnp.int32, (BLK, BLK), 1)
        causal = jnp.where(k_index <= q_index, 0.0, HIDDEN).astype(jnp.float32)
        causal = jnp.concatenate([causal] * ratio, axis=0)
        for h in range(CHUNK_HEADS):
            cols = pl.ds(pl.multiple_of(c * width + h * DH, DH), DH)
            for a in range(blocks):
                own_rows = (a + 1) * BLK

                def gathered(halo_ref, own_ref):
                    parts = []
                    if own_rows < rows:
                        parts.append(halo_ref[0, own_rows:, cols])
                    for r in range(1, window):
                        parts.append(halo_ref[r, :, cols])
                    parts.append(own_ref[:own_rows, cols])
                    return jnp.concatenate(parts, axis=0)

                head_cols = [
                    pl.ds(pl.multiple_of((c * width + h * DH) * ratio + g * DH, DH), DH)
                    for g in range(ratio)
                ]
                tile_rows = slice(a * BLK, (a + 1) * BLK)
                q_tile = jnp.concatenate([q_own[tile_rows, hc] for hc in head_cols], axis=0)
                scores = lax.dot_general(
                    q_tile,
                    gathered(k_halo, k_own),
                    (((1,), (1,)), ((), ())),
                    preferred_element_type=jnp.float32,
                )
                scores = scores + hide_rows[a]
                scores = jnp.concatenate([scores[:, :-BLK], scores[:, -BLK:] + causal], axis=1)
                top = jnp.max(scores, axis=1, keepdims=True)
                weights = jnp.exp2((scores - top) * EXP2_SCALE)
                total = jnp.sum(weights, axis=1, keepdims=True)
                blended = jnp.dot(
                    weights.astype(jnp.bfloat16),
                    gathered(v_halo, v_own),
                    preferred_element_type=jnp.float32,
                )
                blended = (blended / total).astype(o_own.dtype)
                for g in range(ratio):
                    o_own[tile_rows, head_cols[g]] = blended[g * BLK : (g + 1) * BLK]

    def out_copy(c):
        return pltpu.make_async_copy(o_own.at[:, q_cols(c)], o_hbm.at[:, q_cols(c)], out_sem.at[c])

    def arrived(c, slot):
        for copy in remote(c, None, slot, partner):
            copy.wait_recv()

    def step_of(t, carry):
        @pl.when(t < chunks)
        def _():
            c = t
            arrived(c, 0)

            @pl.when(core == 1)
            def _():
                start(remote(c, 0, window - 1, partner))

            for step in range(1, pairs):

                @pl.when(pair + step >= pairs)
                def _():
                    start(remote(c, 0, 2 * step, pair_device(step)))

        @pl.when((t >= 1) & (t < chunks + 1))
        def _():
            c = t - 1
            for step in range(1, pairs):
                arrived(c, 2 * step)
                start(remote(c, 2 * step, partner_slot(step), partner))

        @pl.when((t >= 2) & (t < chunks + 2))
        def _():
            c = t - 2
            for r in range(1, window, 2):
                arrived(c, r)
            attend(c)

        @pl.when(t >= 3)
        def _():
            out_copy(t - 3).start()

        return carry

    lax.fori_loop(0, chunks + 3, step_of, 0)

    def finish(c, carry):
        for slot in range(window):
            for copy in remote(c, None, slot, partner):
                copy.wait_send()
        out_copy(c).wait()
        return carry

    lax.fori_loop(0, chunks, finish, 0)


def on_device(n, queries, keys, values, doc_blocks):
    window = n // 4
    rows, kv_width = keys.shape
    chunks = kv_width // (CHUNK_HEADS * DH)
    return pl.pallas_call(
        functools.partial(kernel, n, window),
        out_shape=jax.ShapeDtypeStruct(queries.shape, queries.dtype),
        in_specs=[pl.BlockSpec(memory_space=pltpu.SMEM)]
        + [pl.BlockSpec(memory_space=pl.ANY)] * 3,
        out_specs=pl.BlockSpec(memory_space=pl.ANY),
        scratch_shapes=[
            pltpu.VMEM(queries.shape, queries.dtype),
            pltpu.VMEM(keys.shape, keys.dtype),
            pltpu.VMEM(values.shape, values.dtype),
            pltpu.VMEM((window, rows, kv_width), keys.dtype),
            pltpu.VMEM((window, rows, kv_width), values.dtype),
            pltpu.VMEM(queries.shape, queries.dtype),
            pltpu.SemaphoreType.DMA((3,)),
            pltpu.SemaphoreType.DMA((chunks,)),
            pltpu.SemaphoreType.DMA((2, window, chunks)),
            pltpu.SemaphoreType.DMA((2, window, chunks)),
        ],
        compiler_params=pltpu.CompilerParams(
            collective_id=0, has_side_effects=True, vmem_limit_bytes=60 * 1024 * 1024
        ),
    )(doc_blocks, queries, keys, values)


def solution(mesh):
    spread = P(("groups", "seq"), None)
    return jax.shard_map(
        functools.partial(on_device, mesh.shape["seq"]),
        mesh=mesh,
        in_specs=(spread, spread, spread, P("groups")),
        out_specs=spread,
        check_vma=False,
    )
```

```python
import functools

import jax
import jax.numpy as jnp
from jax import lax
from jax.experimental import pallas as pl
from jax.experimental.pallas import tpu as pltpu
from jax.sharding import PartitionSpec as P

DH = 128
BLK = 128
CHUNK_HEADS = 1
ROUTED = 1
EXP2_SCALE = 144.0 ** (-0.5) * 1.4426950408889634
HIDDEN = -1e30


def kernel(
    n,
    window,
    docs_ref,
    q_hbm,
    k_hbm,
    v_hbm,
    o_own,
    q_own,
    k_own,
    v_own,
    k_halo,
    v_halo,
    local_sem,
    send_sem,
    recv_sem,
    k_transit,
    v_transit,
    transit_send,
    transit_recv,
    forward_send,
):
    me = lax.axis_index("seq")
    pairs = window // 2
    place = lax.rem(me, window)
    base = me - place
    pair = place // 2
    core = lax.rem(me, 2)
    partner = me + 1 - 2 * core
    above = me + window
    below = me - window
    has_above = above < n
    has_below = below >= 0

    rows, kv_width = k_hbm.shape
    ratio = q_hbm.shape[1] // kv_width
    width = CHUNK_HEADS * DH
    chunks = kv_width // width
    blocks = rows // BLK
    own_hbm = (k_hbm, v_hbm)
    halo = (k_halo, v_halo)
    transit = (k_transit, v_transit)
    first_routed = chunks - ROUTED

    def pair_device(step):
        return base + 2 * lax.rem(pair + step, pairs) + core

    def kv_cols(c):
        return pl.ds(pl.multiple_of(c * width, width), width)

    def remote_one(kind, c, src_slot, dst_slot, device, from_row=0):
        taken = pl.ds(from_row, rows - from_row)
        if src_slot is None:
            src = own_hbm[kind].at[taken, kv_cols(c)]
        else:
            src = halo[kind].at[src_slot, taken, kv_cols(c)]
        return pltpu.make_async_remote_copy(
            src_ref=src,
            dst_ref=halo[kind].at[dst_slot, taken, kv_cols(c)],
            send_sem=send_sem.at[kind, dst_slot, c],
            recv_sem=recv_sem.at[kind, dst_slot, c],
            device_id={"seq": device},
            device_id_type=pl.DeviceIdType.MESH,
        )

    def is_routed(c):
        return (c >= first_routed) & (c < first_routed + ROUTED)

    def turn(spot):
        moved = jnp.where(spot < chunks - 1, spot + 1, first_routed - 1)
        return jnp.where((pair == 0) & (spot >= first_routed - 1), moved, spot)

    def across(kind, c, step):
        spot = c - first_routed
        return pltpu.make_async_remote_copy(
            src_ref=own_hbm[kind].at[:, kv_cols(c)],
            dst_ref=transit[kind].at[step - 1, spot],
            send_sem=transit_send.at[kind, step - 1, spot],
            recv_sem=transit_recv.at[kind, step - 1, spot],
            device_id={"seq": pair_device(step)},
            device_id_type=pl.DeviceIdType.MESH,
        )

    def forward(kind, c, step):
        spot = c - first_routed
        return pltpu.make_async_remote_copy(
            src_ref=transit[kind].at[step - 1, spot],
            dst_ref=halo[kind].at[2 * step, :, kv_cols(c)],
            send_sem=forward_send.at[kind, step - 1, spot],
            recv_sem=recv_sem.at[kind, 2 * step, c],
            device_id={"seq": above},
            device_id_type=pl.DeviceIdType.MESH,
        )

    def remote(c, src_slot, dst_slot, device):
        return [remote_one(kind, c, src_slot, dst_slot, device) for kind in range(2)]

    def upward(kind, c, act):
        @pl.when(place == 0)
        def _():
            act(remote_one(kind, c, None, 0, above, BLK))

        @pl.when(place != 0)
        def _():
            act(remote_one(kind, c, None, 0, above))

    def start(copies):
        for copy in copies:
            copy.start()

    def partner_slot(step):
        return lax.rem(2 * step + 1 - 2 * core + window, window)

    barrier = pltpu.get_barrier_semaphore()

    def greet(device):
        pl.semaphore_signal(
            barrier, inc=1, device_id={"seq": device}, device_id_type=pl.DeviceIdType.MESH
        )

    greet(partner)
    for step in range(1, pairs):
        greet(pair_device(step))

    @pl.when(has_above)
    def _():
        greet(above)

    @pl.when(has_below)
    def _():
        greet(below)

    local = [
        pltpu.make_async_copy(k_hbm, k_own, local_sem.at[0]),
        pltpu.make_async_copy(v_hbm, v_own, local_sem.at[1]),
        pltpu.make_async_copy(q_hbm, q_own, local_sem.at[2]),
    ]
    start(local)
    pl.semaphore_wait(
        barrier, pairs + has_above.astype(jnp.int32) + has_below.astype(jnp.int32)
    )

    def cross_first(spot, carry):
        for step in range(1, pairs):

            @pl.when((pair + step >= pairs) & has_above)
            def _():
                for kind in range(2):
                    across(kind, first_routed + spot, step).start()

        return carry

    lax.fori_loop(0, ROUTED, cross_first, 0)

    def first_sends(c, carry):
        @pl.when(has_above)
        def _():
            for kind in range(2):
                upward(kind, c, lambda copy: copy.start())

        for step in range(1, pairs):

            @pl.when(pair + step < pairs)
            def _():
                start(remote(c, None, 2 * step, pair_device(step)))

        @pl.when(core == 0)
        def _():
            start(remote(c, None, 1, partner))

        return carry

    lax.fori_loop(0, chunks, first_sends, 0)

    @pl.when(jnp.logical_not(has_below))
    def _():
        for r in range(window):

            @pl.when((r == 0) | (r > place))
            def _():
                def clear(i, carry):
                    taken = pl.ds(pl.multiple_of(i * 16, 16), 16)
                    for ref in halo:
                        ref[r, taken, :] = jnp.zeros((16, kv_width), ref.dtype)
                    return carry

                lax.fori_loop(0, rows // 16, clear, 0)

    hide_rows = []
    for a in range(blocks):
        number = me * blocks + a
        end = jnp.int32(0)
        first = jnp.int32(0)
        for d in range(docs_ref.shape[0]):
            end = end + docs_ref[d]
            first = jnp.where(end <= number, end, first)
        held = [(me - window) * blocks + b for b in range(a + 1, blocks)]
        for r in range(1, window):
            held += [(me - r) * blocks + b for b in range(blocks)]
        held += [me * blocks + b for b in range(a + 1)]
        hide_rows.append(
            jnp.concatenate(
                [
                    jnp.full((1, BLK), jnp.where(b >= first, 0.0, HIDDEN), jnp.float32)
                    for b in held
                ],
                axis=1,
            )
        )

    for copy in local:
        copy.wait()

    def attend(c):
        q_index = lax.broadcasted_iota(jnp.int32, (BLK, BLK), 0)
        k_index = lax.broadcasted_iota(jnp.int32, (BLK, BLK), 1)
        causal = jnp.where(k_index <= q_index, 0.0, HIDDEN).astype(jnp.float32)
        causal = jnp.concatenate([causal] * ratio, axis=0)
        for h in range(CHUNK_HEADS):
            cols = pl.ds(pl.multiple_of(c * width + h * DH, DH), DH)
            for a in range(blocks):
                own_rows = (a + 1) * BLK

                def gathered(halo_ref, own_ref):
                    parts = []
                    if own_rows < rows:
                        parts.append(halo_ref[0, own_rows:, cols])
                    for r in range(1, window):
                        parts.append(halo_ref[r, :, cols])
                    parts.append(own_ref[:own_rows, cols])
                    return jnp.concatenate(parts, axis=0)

                head_cols = [
                    pl.ds(pl.multiple_of((c * width + h * DH) * ratio + g * DH, DH), DH)
                    for g in range(ratio)
                ]
                tile_rows = slice(a * BLK, (a + 1) * BLK)
                q_tile = jnp.concatenate([q_own[tile_rows, hc] for hc in head_cols], axis=0)
                scores = lax.dot_general(
                    q_tile,
                    gathered(k_halo, k_own),
                    (((1,), (1,)), ((), ())),
                    preferred_element_type=jnp.float32,
                )
                scores = scores + hide_rows[a]
                scores = jnp.concatenate([scores[:, :-BLK], scores[:, -BLK:] + causal], axis=1)
                top = jnp.max(scores, axis=1, keepdims=True)
                weights = jnp.exp2((scores - top) * EXP2_SCALE)
                total = jnp.sum(weights, axis=1, keepdims=True)
                blended = jnp.dot(
                    weights.astype(jnp.bfloat16),
                    gathered(v_halo, v_own),
                    preferred_element_type=jnp.float32,
                )
                blended = (blended / total).astype(o_own.dtype)
                for g in range(ratio):
                    o_own[tile_rows, head_cols[g]] = blended[g * BLK : (g + 1) * BLK]

    def arrived(c, slot):
        for copy in remote(c, None, slot, partner):
            copy.wait_recv()

    def step_of(t, carry):
        @pl.when((t < chunks) & has_below)
        def _():
            c = t
            for kind in range(2):
                upward(kind, c, lambda copy: copy.wait_recv())

                @pl.when(core == 1)
                def _():
                    remote_one(kind, c, 0, window - 1, partner).start()

                for step in range(1, pairs):

                    @pl.when((pair + step >= pairs) & jnp.logical_not(is_routed(c)))
                    def _():
                        remote_one(kind, c, 0, 2 * step, pair_device(step)).start()

        @pl.when((t < ROUTED) & has_above)
        def _():
            for step in range(1, pairs):

                @pl.when(step > pair)
                def _():
                    for kind in range(2):
                        across(kind, t + first_routed, step).wait_recv()
                        forward(kind, t + first_routed, step).start()

        @pl.when((t >= 1) & (t < chunks + 1))
        def _():
            c = turn(t - 1)
            for step in range(1, pairs):

                @pl.when((pair >= step) | has_below)
                def _():
                    for kind in range(2):
                        remote_one(kind, c, None, 2 * step, partner).wait_recv()
                        remote_one(kind, c, 2 * step, partner_slot(step), partner).start()

        @pl.when((t >= 2) & (t < chunks + 2))
        def _():
            c = turn(t - 2)
            for r in range(1, window, 2):

                @pl.when((place >= r) | has_below)
                def _():
                    arrived(c, r)

            attend(c)

        return carry

    lax.fori_loop(0, chunks + 2, step_of, 0)

    def finish(c, carry):
        def sent(slot):
            for copy in remote(c, None, slot, partner):
                copy.wait_send()

        @pl.when(has_above)
        def _():
            for kind in range(2):
                upward(kind, c, lambda copy: copy.wait_send())

        @pl.when((core == 0) | has_below)
        def _():
            sent(partner_slot(0))

        for step in range(1, pairs):

            @pl.when((pair + step < pairs) | (has_below & jnp.logical_not(is_routed(c))))
            def _():
                sent(2 * step)

            @pl.when((pair + step >= pairs) & has_above & is_routed(c))
            def _():
                for kind in range(2):
                    across(kind, c, step).wait_send()

            @pl.when((step > pair) & has_above & is_routed(c))
            def _():
                for kind in range(2):
                    forward(kind, c, step).wait_send()

            @pl.when((pair >= step) | has_below)
            def _():
                sent(partner_slot(step))

        return carry

    lax.fori_loop(0, chunks, finish, 0)


def on_device(n, queries, keys, values, doc_blocks):
    window = n // 4
    rows, kv_width = keys.shape
    chunks = kv_width // (CHUNK_HEADS * DH)
    return pl.pallas_call(
        functools.partial(kernel, n, window),
        out_shape=pltpu.VMEM(queries.shape, queries.dtype),
        in_specs=[pl.BlockSpec(memory_space=pltpu.SMEM)]
        + [pl.BlockSpec(memory_space=pl.ANY)] * 3,
        out_specs=pl.BlockSpec(memory_space=pltpu.VMEM),
        scratch_shapes=[
            pltpu.VMEM(queries.shape, queries.dtype),
            pltpu.VMEM(keys.shape, keys.dtype),
            pltpu.VMEM(values.shape, values.dtype),
            pltpu.VMEM((window, rows, kv_width), keys.dtype),
            pltpu.VMEM((window, rows, kv_width), values.dtype),
            pltpu.SemaphoreType.DMA((3,)),
            pltpu.SemaphoreType.DMA((2, window, chunks)),
            pltpu.SemaphoreType.DMA((2, window, chunks)),
            pltpu.VMEM((window // 2 - 1, ROUTED, rows, CHUNK_HEADS * DH), keys.dtype),
            pltpu.VMEM((window // 2 - 1, ROUTED, rows, CHUNK_HEADS * DH), values.dtype),
            pltpu.SemaphoreType.DMA((2, window // 2 - 1, ROUTED)),
            pltpu.SemaphoreType.DMA((2, window // 2 - 1, ROUTED)),
            pltpu.SemaphoreType.DMA((2, window // 2 - 1, ROUTED)),
        ],
        compiler_params=pltpu.CompilerParams(
            collective_id=0, has_side_effects=True, vmem_limit_bytes=60 * 1024 * 1024
        ),
    )(doc_blocks, queries, keys, values)


def solution(mesh):
    spread = P(("groups", "seq"), None)
    return jax.shard_map(
        functools.partial(on_device, mesh.shape["seq"]),
        mesh=mesh,
        in_specs=(spread, spread, spread, P("groups")),
        out_specs=spread,
        check_vma=False,
    )
```
